32 devices in a mesh: ctx: 16 (over z, x, core), head: 2 (over y).
Axes of the slice: x: 2, y: 2, z: 4, core: 2. Of those that a mesh axis runs over, the one named last changes fastest.
Arguments:
- queries: bfloat16 [4096, 32, 128], P('ctx', 'head'), may hold values from -300 to 300
- key_rows: bfloat16 [4096, 4, 128], P('ctx', 'head'), may hold values from -6 to 6
- value_vectors: bfloat16 [4096, 4, 128], P('ctx', 'head'), may hold values from -6 to 6
- doc_ids: int32 [4096], replicated, may hold values from 0 to 2, never falling along the last dimension, each value on 1 to 1792 neighbouring positions
Outputs:
- attended: bfloat16 [4096, 32, 128], P(('ctx', 'head'))
The draws below stay inside these ranges and needn't reach their ends.
Inputs may be any that keep to these rules, and one draw needn't show every extreme that they name: `doc_ids`: ids never fall along the pack and each prompt holds at most 1792 tokens.
All inputs are finite; a program needn't handle non-finite values.
Results may differ from the reference program's by a relative error of at most 0.008.
Values may be sent and summed in bfloat16 or wider, within the bound.
A program may use at most 64 MiB of HBM per device.

```python
import math
import jax
import jax.numpy as jnp
import numpy as np
from jax import lax

QUERY_HEADS = 32
KEY_VALUE_HEADS = 4
HEAD_SIZE = 128
TOKENS_PER_SHARD = 256
PROMPTS = 3
REACH = 7
PACKED_TOKENS = 4096
N_CTX = 16


def drawn_pair(key):
    key_sample = jax.random.fold_in(key, 11)
    query_draw = jax.random.fold_in(key, 23)
    key_entries = jnp.clip(jax.random.normal(key_sample, (PACKED_TOKENS, KEY_VALUE_HEADS, HEAD_SIZE), jnp.float32), -6.0, 6.0)
    query_vals = jnp.clip(jax.random.normal(query_draw, (PACKED_TOKENS, QUERY_HEADS, HEAD_SIZE), jnp.float32), -6.0, 6.0)
    return (query_vals, key_entries)


def draw_queries(key, part):
    return drawn_pair(key)[0].astype(jnp.bfloat16)


def draw_key_rows(key, part):
    return drawn_pair(key)[1].astype(jnp.bfloat16)


def steps_of(stream_key, dims, shards, smallest, largest):
    loudness = 1.0
    for dim, parts in shards:
        draws = jax.random.uniform(jax.random.fold_in(jax.random.fold_in(stream_key, 6), dim), (parts,), jnp.float32, smallest / len(shards), largest / len(shards))
        loudness = loudness * jnp.repeat(jnp.exp(draws), dims[dim] // parts).reshape((-1,) + (1,) * (len(dims) - 1 - dim))
    return loudness


def split_up(count, total, reach, lean):
    weights = [(1 << 20) // math.isqrt(rank ** lean) + 1 for rank in range(2, count + 1)]
    spare, given = total - reach - (count - 1), [1] * (count - 1)
    while spare > 0:
        candidates = [i for i in range(count - 1) if given[i] < reach]
        pool, left = sum([weights[i] for i in candidates]), spare
        for i in candidates:
            more = min(reach - given[i], max(1, left * weights[i] // pool), spare)
            given[i] = given[i] + more
            spare = spare - more
    return np.array([reach] + given)


def uneven(stream_key, count, total, limit, skew):
    if count == 2:
        one = jax.random.randint(stream_key, (), max(1, total - limit), min(limit, total - 1) + 1)
        return jnp.stack([one, total - one])
    lengths = jnp.asarray(split_up(count, total, limit, skew), jnp.int32)
    twos = (count - 1) // 2
    giver, taker = lengths[1:1 + 2 * twos:2], lengths[2:2 + 2 * twos:2]
    margin = jnp.minimum(giver - 1, limit - taker)
    shifted = jax.random.randint(jax.random.fold_in(stream_key, 1), (twos,), 0, 1 << 20) % (margin + 1)
    lengths = lengths.at[1:1 + 2 * twos:2].set(giver - shifted).at[2:2 + 2 * twos:2].set(taker + shifted)
    return lengths[jax.random.permutation(jax.random.fold_in(stream_key, 2), count)]


def noise(own_key, dims, scale, most, cuts=(), kind=jnp.bfloat16):
    loudness = steps_of(own_key, dims, cuts, -0.22, 0.18) if cuts else 1.0
    result = jax.random.normal(own_key, dims, jnp.float32) * scale * loudness
    return jnp.minimum(jnp.maximum(result, -most), most).astype(kind)


def setup_inputs(seed: int = 0) -> dict:
    key_of = jax.random.split(jax.random.key(seed), 5)
    return {
        "queries": draw_queries(jax.random.fold_in(key_of[4], 71), 0),
        "key_rows": draw_key_rows(jax.random.fold_in(key_of[4], 71), 0),
        "value_vectors": noise(key_of[2], (PACKED_TOKENS, KEY_VALUE_HEADS, HEAD_SIZE), 1.0, 6.0, ((0, 16), (1, 2))),
        "doc_ids": jnp.searchsorted(jnp.cumsum(uneven(key_of[3], PROMPTS, PACKED_TOKENS, REACH * TOKENS_PER_SHARD, 2)), jnp.arange(PACKED_TOKENS), side="right").astype(jnp.int32),
    }


def reference(queries, key_rows, value_vectors, doc_ids):
    head_group = QUERY_HEADS // KEY_VALUE_HEADS
    window = (REACH + 1) * TOKENS_PER_SHARD
    inv_root = HEAD_SIZE ** -0.5

    def query_block(block_num):
        query_offset = (block_num * TOKENS_PER_SHARD).astype(jnp.int32)
        k_start = jnp.maximum(query_offset - REACH * TOKENS_PER_SHARD, 0).astype(jnp.int32)
        query_portion = lax.dynamic_slice_in_dim(queries, query_offset, TOKENS_PER_SHARD, 0).reshape(TOKENS_PER_SHARD, KEY_VALUE_HEADS, head_group, HEAD_SIZE).astype(jnp.float32)
        k_part = lax.dynamic_slice_in_dim(key_rows, k_start, window, 0).astype(jnp.float32)
        v_part = lax.dynamic_slice_in_dim(value_vectors, k_start, window, 0).astype(jnp.float32)
        q_doc = lax.dynamic_slice_in_dim(doc_ids, query_offset, TOKENS_PER_SHARD, 0)
        k_doc = lax.dynamic_slice_in_dim(doc_ids, k_start, window, 0)
        q_pos = query_offset + jnp.arange(TOKENS_PER_SHARD, dtype=jnp.int32)
        k_pos = k_start + jnp.arange(window, dtype=jnp.int32)
        visible = (q_doc[:, None] == k_doc[None, :]) & (k_pos[None, :] <= q_pos[:, None])
        scores = jnp.einsum('tgrd,ugd->grtu', query_portion, k_part) * inv_root
        masked = jnp.where(visible, scores, -jnp.inf)
        row_max = jnp.max(masked, axis=-1, keepdims=True)
        weights = jnp.where(visible, jnp.exp(scores - row_max), 0.0)
        total = jnp.sum(weights, axis=-1, keepdims=True)
        rounded = lax.optimization_barrier(weights.astype(jnp.bfloat16)).astype(jnp.float32)
        summed = jnp.einsum('grtu,ugd->grtd', rounded, v_part) / total
        return summed.transpose(2, 0, 1, 3).reshape(TOKENS_PER_SHARD, QUERY_HEADS, HEAD_SIZE).astype(jnp.bfloat16)

    blocks = lax.map(query_block, jnp.arange(N_CTX, dtype=jnp.int32))
    return blocks.reshape(PACKED_TOKENS, QUERY_HEADS, HEAD_SIZE)
```

```python
import functools
import math

import jax
import jax.numpy as jnp
from jax import lax
from jax.experimental import pallas as pl
from jax.experimental.pallas import tpu as pltpu
from jax.sharding import PartitionSpec as P

MESH = pl.DeviceIdType.MESH
MEMBERS = 4
CHUNK_BLOCKS = 4
ROWS = 256
HIDDEN = -1e30


def kernel(n, q_ref, kv_ref, start_ref, out_ref, win, q_scr, start_scr, done,
           ring_send, pair_send, core_send, recv, local_sem, out_send, out_recv):
    reach = n // 2 - 1
    groups = n // MEMBERS
    depth = -(-reach // MEMBERS)
    kv_heads = kv_ref.shape[0]
    tok_len = q_ref.shape[0]
    head_dim = q_ref.shape[2]
    group_heads = q_ref.shape[1] // kv_heads
    half = tok_len // 2
    scale = head_dim ** (-0.5) * math.log2(math.e)

    i = lax.axis_index("ctx")
    y = lax.axis_index("head")
    g = i // MEMBERS
    j = i % MEMBERS
    x = j // 2
    k = j % 2
    own = MEMBERS * depth + j
    first = own - reach
    after = lax.rem(i + MEMBERS, n)
    before = lax.rem(i + n - MEMBERS, n)
    pair = i + 2 - 4 * x
    sibling = i + 1 - 2 * k

    barrier = pltpu.get_barrier_semaphore()
    for target in (after, before, pair, sibling):
        pl.semaphore_signal(barrier, inc=1, device_id={"ctx": target}, device_id_type=MESH)
    pl.semaphore_signal(barrier, inc=1, device_id={"head": 1 - y}, device_id_type=MESH)
    pl.semaphore_wait(barrier, 5)

    def slot(s, m):
        return MEMBERS * (depth - s) + m

    def copy(src, lin, h, sem, target):
        return pltpu.make_async_remote_copy(
            src_ref=src, dst_ref=win.at[lin, h], send_sem=sem, recv_sem=recv.at[lin, h],
            device_id={"ctx": target}, device_id_type=MESH)

    def source(s, m, h):
        return kv_ref.at[h] if s is None else win.at[slot(s, m), h]

    base = MEMBERS * depth

    def ring_wanted(s):
        return slot(s, j) >= base - reach

    def pair_wanted(s, m, chip):
        lin = slot(s, m)
        return (lin >= base + 2 * chip - reach) & (lin < base + 2 * chip) & (g >= s)

    def core_wanted(s, m, core):
        lin = slot(s, m)
        mine = base + 2 * x + core
        return (lin >= mine - reach) & (lin < mine) & (g >= s)

    def send_ring(s, h, src, act):
        @pl.when((g + 1 < groups) & (g >= s) & ring_wanted(s + 1))
        def _():
            c = copy(src, slot(s + 1, j), h, ring_send.at[s, h], after)
            act(c)

    def send_pair(s, h, src, act):
        @pl.when(pair_wanted(s, j, 1 - x))
        def _():
            act(copy(src, slot(s, j), h, pair_send.at[s, h], pair))

    def send_core(s, m, way, h, src, act):
        @pl.when(core_wanted(s, m, 1 - k))
        def _():
            act(copy(src, slot(s, m), h, core_send.at[way, s, h], sibling))

    def start(c):
        c.start()

    def wait_sent(c):
        c.wait_send()

    def wait_slot(lin, h):
        copy(win.at[lin, h], lin, h, ring_send.at[0, h], sibling).wait_recv()

    def pump_own(h):
        send_ring(0, h, kv_ref.at[h], start)
        send_pair(0, h, kv_ref.at[h], start)
        send_core(0, j, 0, h, kv_ref.at[h], start)

    def pump_ring(s, h):
        @pl.when((g >= s) & ring_wanted(s))
        def _():
            wait_slot(slot(s, j), h)
        src = win.at[slot(s, j), h]
        if s < depth:
            send_ring(s, h, src, start)
        send_pair(s, h, src, start)
        send_core(s, j, 0, h, src, start)

    def pump_pair(s, h):
        m = j + 2 - 4 * x

        @pl.when(pair_wanted(s, m, x))
        def _():
            wait_slot(slot(s, m), h)
        send_core(s, m, 1, h, win.at[slot(s, m), h], start)

    def pump_core(h):
        for s in range(depth + 1):
            for m in (j + 1 - 2 * k, 3 - j):
                @pl.when(core_wanted(s, m, k))
                def _():
                    wait_slot(slot(s, m), h)

    def stages(h):
        result = []
        for s in range(1, depth + 1):
            result.append(functools.partial(pump_ring, s, h))
            result.append(functools.partial(pump_pair, s - 1, h))
        result.append(functools.partial(pump_pair, depth, h))
        result.append(functools.partial(pump_core, h))
        return result

    for h in range(kv_heads):
        pump_own(h)
        pltpu.make_async_copy(kv_ref.at[h], win.at[own, h], local_sem.at[h]).start()

    def clear(d, _):
        @pl.when(i < d)
        def _():
            win[own - d] = jnp.zeros(win.shape[1:], win.dtype)
        return 0
    lax.fori_loop(1, reach + 1, clear, 0)

    rows_total = tok_len * group_heads
    toks = ROWS // group_heads

    def prepare(b, _):
        t = pl.multiple_of(b * toks, toks)
        r = pl.multiple_of(b * ROWS, ROWS)
        q = q_ref[pl.ds(t, toks)].astype(jnp.float32)
        for h in range(kv_heads):
            part = q[:, h * group_heads:(h + 1) * group_heads].reshape(ROWS, head_dim)
            q_scr[h, pl.ds(r, ROWS), :] = part.astype(q_scr.dtype)
        st = start_ref[pl.ds(t, toks), :]
        start_scr[pl.ds(r, ROWS), :] = jnp.broadcast_to(
            st[:, None, :], (toks, group_heads, 128)).reshape(ROWS, 128)
        return 0
    lax.fori_loop(0, rows_total // ROWS, prepare, 0)

    chunks = (reach + 1) // CHUNK_BLOCKS
    width = CHUNK_BLOCKS * tok_len
    lane = lax.broadcasted_iota(jnp.int32, (ROWS, 128), 1)
    row_tok = lax.broadcasted_iota(jnp.int32, (ROWS, 128), 0) // group_heads

    def attend(h, r, chunk, newest, state):
        q = q_scr[h, pl.ds(r, ROWS), :]
        begin = first + chunk * CHUNK_BLOCKS
        key_base = (i - reach + chunk * CHUNK_BLOCKS) * tok_len
        st = start_scr[pl.ds(r, ROWS), :] - key_base - lane
        tiles = []
        for b in range(CHUNK_BLOCKS):
            keys = win[begin + b, h, 0]
            s = lax.dot_general(q, keys, (((1,), (1,)), ((), ())),
                                preferred_element_type=jnp.float32)
            for c in range(tok_len // 128):
                off = b * tok_len + c * 128
                tile = s[:, c * 128:(c + 1) * 128]
                seen = st <= off
                if newest and b == CHUNK_BLOCKS - 1:
                    seen = seen & (lane + c * 128 <= row_tok + r // group_heads)
                tiles.append(jnp.where(seen, tile, HIDDEN))
        top = functools.reduce(jnp.maximum, tiles)
        top = jnp.max(top, axis=1, keepdims=True)
        if state is not None:
            top = jnp.maximum(top, state[0])
        weights = [jnp.exp2((t - top) * scale) for t in tiles]
        total = functools.reduce(jnp.add, weights)
        values = win[pl.ds(begin, CHUNK_BLOCKS), h, 1].reshape(width, head_dim)
        packed = jnp.concatenate([w.astype(jnp.bfloat16) for w in weights], axis=1)
        product = jnp.dot(packed, values, preferred_element_type=jnp.float32)
        if state is None:
            return top, total, product
        rescale = jnp.exp2((state[0] - top) * scale)
        return top, state[1] * rescale + total, state[2] * rescale + product

    def block(h, r):
        state = attend(h, r, chunks - 1, True, None)
        if chunks == 2:
            state = attend(h, r, 0, False, state)
        else:
            state = lax.fori_loop(
                1, chunks, lambda c, st: attend(h, r, chunks - 1 - c, False, st), state)
        total = jnp.sum(state[1], axis=1, keepdims=True)
        return (state[2] / total).reshape(toks, group_heads, head_dim).astype(jnp.bfloat16)

    blocks_half = half // toks

    def rows_of(h, token0, dst, b):
        t = pl.multiple_of(token0 + b * toks, toks)
        r = pl.multiple_of(t * group_heads, ROWS)
        dst(pl.multiple_of(b * toks, toks), block(h, r))

    def store_sent(h, t, value):
        done[h, pl.ds(t, toks)] = value

    def store_own(h, t, value):
        out_ref[y, h, pl.ds(t, toks)] = value

    def out_copy(h):
        return pltpu.make_async_remote_copy(
            src_ref=done.at[h], dst_ref=out_ref.at[y, h], send_sem=out_send.at[h],
            recv_sem=out_recv.at[h], device_id={"head": 1 - y}, device_id_type=MESH)

    for h in range(kv_heads):
        pltpu.make_async_copy(kv_ref.at[h], win.at[own, h], local_sem.at[h]).wait()
    for stage in stages(0):
        stage()
    for h in range(kv_heads):
        pending = stages(h + 1) if h + 1 < kv_heads else []
        per = -(-len(pending) // (2 * blocks_half))
        for part, (token0, store) in enumerate(
                (((1 - y) * half, store_sent), (y * half, store_own))):
            if pending:
                for b in range(blocks_half):
                    rows_of(h, token0, functools.partial(store, h), b)
                    for stage in pending[:per]:
                        stage()
                    pending = pending[per:]
            else:
                def step(b, _):
                    rows_of(h, token0, functools.partial(store, h), b)
                    return 0
                lax.fori_loop(0, blocks_half, step, 0)
            if part == 0:
                out_copy(h).start()
        for stage in pending:
            stage()

    for h in range(kv_heads):
        send_ring(0, h, kv_ref.at[h], wait_sent)
        for s in range(depth + 1):
            src = win.at[slot(s, j), h]
            if 0 < s < depth:
                send_ring(s, h, src, wait_sent)
            send_pair(s, h, src, wait_sent)
            send_core(s, j, 0, h, src, wait_sent)
            m = j + 2 - 4 * x
            send_core(s, m, 1, h, win.at[slot(s, m), h], wait_sent)
        out_copy(h).wait()


def body(n, queries, key_rows, value_vectors, doc_ids):
    tok_len, heads_here, head_dim = queries.shape
    kv_heads = key_rows.shape[1]
    group_heads = heads_here // kv_heads
    reach = n // 2 - 1
    depth = -(-reach // MEMBERS)
    slots = MEMBERS * (depth + 1)
    kv = jnp.stack([key_rows, value_vectors]).transpose(2, 0, 1, 3)
    i = lax.axis_index("ctx")
    own_doc = lax.dynamic_slice_in_dim(doc_ids, i * tok_len, tok_len, 0)
    begins = jnp.sum((doc_ids[None, :] < own_doc[:, None]).astype(jnp.int32), axis=1)
    begins = jnp.broadcast_to(begins[:, None], (tok_len, 128))
    half = tok_len // 2
    dma = pltpu.SemaphoreType.DMA
    out = pl.pallas_call(
        functools.partial(kernel, n),
        out_shape=jax.ShapeDtypeStruct(
            (2, kv_heads, half, group_heads, head_dim), jnp.bfloat16),
        in_specs=[pl.BlockSpec(memory_space=pltpu.VMEM)] * 3,
        out_specs=pl.BlockSpec(memory_space=pltpu.VMEM),
        scratch_shapes=[
            pltpu.VMEM((slots, kv_heads, 2, tok_len, head_dim), jnp.bfloat16),
            pltpu.VMEM((kv_heads, tok_len * group_heads, head_dim), jnp.bfloat16),
            pltpu.VMEM((tok_len * group_heads, 128), jnp.int32),
            pltpu.VMEM((kv_heads, half, group_heads, head_dim), jnp.bfloat16),
            dma((depth, kv_heads)),
            dma((depth + 1, kv_heads)),
            dma((2, depth + 1, kv_heads)),
            dma((slots, kv_heads)),
            dma((kv_heads,)),
            dma((kv_heads,)),
            dma((kv_heads,)),
        ],
        compiler_params=pltpu.CompilerParams(collective_id=0, has_side_effects=True),
    )(queries, kv, begins)
    return out.transpose(2, 0, 1, 3, 4).reshape(half, 2 * heads_here, head_dim)


def solution(mesh):
    placed = (P("ctx", "head", None), P("ctx", "head", None), P("ctx", "head", None), P())
    return jax.shard_map(
        functools.partial(body, mesh.shape["ctx"]), mesh=mesh, in_specs=placed,
        out_specs=P(("ctx", "head"), None, None), check_vma=False,
    )
```

```python
import functools
import math

import jax
import jax.numpy as jnp
from jax import lax
from jax.experimental import pallas as pl
from jax.experimental.pallas import tpu as pltpu
from jax.sharding import PartitionSpec as P

MESH = pl.DeviceIdType.MESH
MEMBERS = 4
CHUNK_BLOCKS = 4
ROWS = 512
HIDDEN = -1e30


def kernel(n, q_ref, kv_ref, docs_ref, out_ref, win, q_scr, start_tok, start_scr, done, top_scr, total_scr, sum_scr,
           ring_send, pair_send, core_send, recv, local_sem, out_send, out_recv):
    reach = n // 2 - 1
    groups = n // MEMBERS
    depth = -(-reach // MEMBERS)
    pieces = kv_ref.shape[0]
    kv_heads = pieces // 2
    tok_len = q_ref.shape[0]
    head_dim = q_ref.shape[2]
    group_heads = q_ref.shape[1] // kv_heads
    half = tok_len // 2
    scale = head_dim ** (-0.5) * math.log2(math.e)

    i = lax.axis_index("ctx")
    y = lax.axis_index("head")
    g = i // MEMBERS
    j = i % MEMBERS
    x = j // 2
    k = j % 2
    own = MEMBERS * depth + j
    first = own - reach
    after = lax.rem(i + MEMBERS, n)
    before = lax.rem(i + n - MEMBERS, n)
    pair = i + 2 - 4 * x
    sibling = i + 1 - 2 * k

    barrier = pltpu.get_barrier_semaphore()
    for target in (after, before, pair, sibling):
        pl.semaphore_signal(barrier, inc=1, device_id={"ctx": target}, device_id_type=MESH)
    pl.semaphore_signal(barrier, inc=1, device_id={"head": 1 - y}, device_id_type=MESH)
    pl.semaphore_wait(barrier, 5)

    def slot(s, m):
        return MEMBERS * (depth - s) + m

    def copy(src, lin, h, sem, target):
        return pltpu.make_async_remote_copy(
            src_ref=src, dst_ref=win.at[lin, h], send_sem=sem, recv_sem=recv.at[lin, h],
            device_id={"ctx": target}, device_id_type=MESH)

    def source(s, m, h):
        return kv_ref.at[h] if s is None else win.at[slot(s, m), h]

    base = MEMBERS * depth

    def ring_wanted(s):
        return slot(s, j) >= base - reach

    def pair_wanted(s, m, chip):
        lin = slot(s, m)
        return (lin >= base + 2 * chip - reach) & (lin < base + 2 * chip) & (g >= s)

    def core_wanted(s, m, core):
        lin = slot(s, m)
        mine = base + 2 * x + core
        return (lin >= mine - reach) & (lin < mine) & (g >= s)

    def send_ring(s, h, src, act):
        @pl.when((g + 1 < groups) & (g >= s) & ring_wanted(s + 1))
        def _():
            c = copy(src, slot(s + 1, j), h, ring_send.at[s, h], after)
            act(c)

    def send_pair(s, h, src, act):
        @pl.when(pair_wanted(s, j, 1 - x))
        def _():
            act(copy(src, slot(s, j), h, pair_send.at[s, h], pair))

    def send_core(s, m, way, h, src, act):
        @pl.when(core_wanted(s, m, 1 - k))
        def _():
            act(copy(src, slot(s, m), h, core_send.at[way, s, h], sibling))

    def start(c):
        c.start()

    def wait_sent(c):
        c.wait_send()

    def wait_slot(lin, h):
        copy(win.at[lin, h], lin, h, ring_send.at[0, h], sibling).wait_recv()

    def pump_own(h):
        send_ring(0, h, kv_ref.at[h], start)
        send_pair(0, h, kv_ref.at[h], start)
        send_core(0, j, 0, h, kv_ref.at[h], start)

    def pump_ring(s, h):
        @pl.when((g >= s) & ring_wanted(s))
        def _():
            wait_slot(slot(s, j), h)
        src = win.at[slot(s, j), h]
        if s < depth:
            send_ring(s, h, src, start)
        send_pair(s, h, src, start)
        send_core(s, j, 0, h, src, start)

    def pump_pair(s, h):
        m = j + 2 - 4 * x

        @pl.when(pair_wanted(s, m, x))
        def _():
            wait_slot(slot(s, m), h)
        send_core(s, m, 1, h, win.at[slot(s, m), h], start)

    def pump_core(s, h):
        for m in (j + 1 - 2 * k, 3 - j):
            @pl.when(core_wanted(s, m, k))
            def _():
                wait_slot(slot(s, m), h)

    def both(act, s, h):
        return [functools.partial(act, s, 2 * h), functools.partial(act, s, 2 * h + 1)]

    def stages(h):
        early = (both(pump_ring, 1, h) + both(pump_pair, 0, h) + both(pump_pair, 1, h)
                 + both(pump_core, 0, h) + both(pump_core, 1, h))
        late = []
        for s in range(2, depth + 1):
            late += [both(pump_ring, s, h), both(pump_pair, s, h)]
        late += [sum([both(pump_core, s, h) for s in range(2, depth + 1)], [])]
        return early, late

    for p in range(pieces):
        pltpu.make_async_copy(kv_ref.at[p], win.at[own, p], local_sem.at[p]).start()
    for p in range(2):
        pump_own(p)

    def clear(d, _):
        @pl.when(i < d)
        def _():
            win[own - d] = jnp.zeros(win.shape[1:], win.dtype)
        return 0
    lax.fori_loop(1, reach + 1, clear, 0)

    rows_total = tok_len * group_heads
    toks = ROWS // group_heads

    for c in range(tok_len // 128):
        ids = docs_ref[pl.ds(i * (tok_len // 128) + c, 1), :].astype(jnp.float32)
        mine = jnp.broadcast_to(ids, (128, 128)).T

        def count(r, smaller):
            other = docs_ref[pl.ds(r, 1), :].astype(jnp.float32)
            return smaller + jnp.where(other < mine, 1.0, 0.0)
        smaller = lax.fori_loop(
            0, docs_ref.shape[0], count, jnp.zeros((128, 128), jnp.float32), unroll=4)
        begin_at = jnp.sum(smaller, axis=1, keepdims=True).astype(jnp.int32)
        start_tok[pl.ds(c * 128, 128), :] = jnp.broadcast_to(begin_at, (128, 128))

    def prepare(b, _):
        t = pl.multiple_of(b * toks, toks)
        r = pl.multiple_of(b * ROWS, ROWS)
        q = q_ref[pl.ds(t, toks)].astype(jnp.float32)
        for h in range(kv_heads):
            part = q[:, h * group_heads:(h + 1) * group_heads].reshape(ROWS, head_dim)
            q_scr[h, pl.ds(r, ROWS), :] = part.astype(q_scr.dtype)
        st = start_tok[pl.ds(t, toks), :]
        start_scr[pl.ds(r, ROWS), :] = jnp.broadcast_to(
            st[:, None, :], (toks, group_heads, 128)).reshape(ROWS, 128)
        return 0
    lax.fori_loop(0, rows_total // ROWS, prepare, 0)

    chunks = (reach + 1) // CHUNK_BLOCKS
    width = CHUNK_BLOCKS * tok_len
    lane = lax.broadcasted_iota(jnp.int32, (ROWS, 128), 1)
    row_tok = lax.broadcasted_iota(jnp.int32, (ROWS, 128), 0) // group_heads

    def attend(h, r, chunk, newest, state):
        q = q_scr[h, pl.ds(r, ROWS), :]
        begin = first + chunk * CHUNK_BLOCKS
        key_base = (i - reach + chunk * CHUNK_BLOCKS) * tok_len
        st = start_scr[pl.ds(r, ROWS), :] - key_base - lane
        tiles = []
        for b in range(CHUNK_BLOCKS):
            keys = win[begin + b, 2 * h]
            s = lax.dot_general(q, keys, (((1,), (1,)), ((), ())),
                                preferred_element_type=jnp.float32)
            for c in range(tok_len // 128):
                off = b * tok_len + c * 128
                tile = s[:, c * 128:(c + 1) * 128]
                seen = st <= off
                if newest and b == CHUNK_BLOCKS - 1:
                    seen = seen & (lane + c * 128 <= row_tok + r // group_heads)
                tiles.append(jnp.where(seen, tile, HIDDEN))
        top = functools.reduce(jnp.maximum, tiles)
        top = jnp.broadcast_to(jnp.max(top, axis=1, keepdims=True), (ROWS, 128))
        if state is not None:
            top = jnp.maximum(top, state[0])
        weights = [jnp.exp2((t - top) * scale) for t in tiles]
        total = functools.reduce(jnp.add, weights)
        values = win[pl.ds(begin, CHUNK_BLOCKS), 2 * h + 1].reshape(width, head_dim)
        packed = jnp.concatenate([w.astype(jnp.bfloat16) for w in weights], axis=1)
        product = jnp.dot(packed, values, preferred_element_type=jnp.float32)
        if state is None:
            return top, total, product
        rescale = jnp.exp2((state[0] - top) * scale)
        return top, state[1] * rescale + total, state[2] * rescale + product

    def begin_rows(h, r):
        state = attend(h, r, chunks - 1, True, None)
        at = pl.ds(r, ROWS)
        top_scr[at, :] = state[0]
        total_scr[at, :] = state[1]
        sum_scr[at, :] = state[2]

    def kept(r):
        at = pl.ds(r, ROWS)
        return top_scr[at, :], total_scr[at, :], sum_scr[at, :]

    def block(h, r, state):
        if state is None:
            state = attend(h, r, chunks - 1, True, None)
        if chunks == 2:
            state = attend(h, r, 0, False, state)
        else:
            state = lax.fori_loop(
                1, chunks, lambda c, st: attend(h, r, chunks - 1 - c, False, st), state)
        total = jnp.sum(state[1], axis=1, keepdims=True)
        return (state[2] / total).reshape(toks, group_heads, head_dim).astype(jnp.bfloat16)

    blocks_half = half // toks

    def rows_of(h, token0, dst, b):
        t = pl.multiple_of(token0 + b * toks, toks)
        r = pl.multiple_of(t * group_heads, ROWS)
        dst(pl.multiple_of(b * toks, toks), block(h, r, kept(r) if h == 0 else None))

    def store_sent(h, t, value):
        done[h, pl.ds(t, toks)] = value

    def store_own(h, t, value):
        out_ref[y, h, pl.ds(t, toks)] = value

    def out_copy(h):
        return pltpu.make_async_remote_copy(
            src_ref=done.at[h], dst_ref=out_ref.at[y, h], send_sem=out_send.at[h],
            recv_sem=out_recv.at[h], device_id={"head": 1 - y}, device_id_type=MESH)

    for p in range(pieces):
        pltpu.make_async_copy(kv_ref.at[p], win.at[own, p], local_sem.at[p]).wait()
    early, late = stages(0)
    for number, stage in enumerate(early):
        stage()
        if number == 1:
            for p in range(2, pieces):
                pump_own(p)

    def spread(groups_of_stages, places):
        per = -(-len(groups_of_stages) // places)
        return [sum(groups_of_stages[c * per:(c + 1) * per], []) for c in range(places)]

    def whole(h):
        order = []
        for s in range(1, depth + 1):
            order += [both(pump_ring, s, h), both(pump_pair, s - 1, h)]
        order += [both(pump_pair, depth, h)]
        return order + [sum([both(pump_core, s, h) for s in range(depth + 1)], [])]

    row_blocks = rows_total // ROWS
    following = [[]] + spread(whole(1), 2 * row_blocks - 1)
    for b, now in enumerate(spread(late, row_blocks)):
        begin_rows(0, b * ROWS)
        for stage in following[b] + now:
            stage()

    for h in range(kv_heads):
        if h == 0:
            pending = following[row_blocks:]
        elif h + 1 < kv_heads:
            pending = spread(whole(h + 1), row_blocks)
        else:
            pending = [[]] * row_blocks
        for part, (token0, store) in enumerate(
                (((1 - y) * half, store_sent), (y * half, store_own))):
            for b in range(blocks_half):
                rows_of(h, token0, functools.partial(store, h), b)
                if part == 0 and b == blocks_half - 1:
                    out_copy(h).start()
                for stage in pending[part * blocks_half + b]:
                    stage()

    for h in range(pieces):
        send_ring(0, h, kv_ref.at[h], wait_sent)
        for s in range(depth + 1):
            src = win.at[slot(s, j), h]
            if 0 < s < depth:
                send_ring(s, h, src, wait_sent)
            send_pair(s, h, src, wait_sent)
            send_core(s, j, 0, h, src, wait_sent)
            m = j + 2 - 4 * x
            send_core(s, m, 1, h, win.at[slot(s, m), h], wait_sent)
    for h in range(kv_heads):
        out_copy(h).wait()


def body(n, queries, key_rows, value_vectors, doc_ids):
    tok_len, heads_here, head_dim = queries.shape
    kv_heads = key_rows.shape[1]
    group_heads = heads_here // kv_heads
    reach = n // 2 - 1
    depth = -(-reach // MEMBERS)
    slots = MEMBERS * (depth + 1)
    kv = jnp.stack([key_rows, value_vectors]).transpose(2, 0, 1, 3)
    pieces = 2 * kv_heads
    kv = kv.reshape(pieces, tok_len, head_dim)
    half = tok_len // 2
    dma = pltpu.SemaphoreType.DMA
    out = pl.pallas_call(
        functools.partial(kernel, n),
        out_shape=jax.ShapeDtypeStruct(
            (2, kv_heads, half, group_heads, head_dim), jnp.bfloat16),
        in_specs=[pl.BlockSpec(memory_space=pltpu.VMEM)] * 3,
        out_specs=pl.BlockSpec(memory_space=pltpu.VMEM),
        scratch_shapes=[
            pltpu.VMEM((slots, pieces, tok_len, head_dim), jnp.bfloat16),
            pltpu.VMEM((kv_heads, tok_len * group_heads, head_dim), jnp.bfloat16),
            pltpu.VMEM((tok_len, 128), jnp.int32),
            pltpu.VMEM((tok_len * group_heads, 128), jnp.int32),
            pltpu.VMEM((kv_heads, half, group_heads, head_dim), jnp.bfloat16),
            pltpu.VMEM((tok_len * group_heads, 128), jnp.float32),
            pltpu.VMEM((tok_len * group_heads, 128), jnp.float32),
            pltpu.VMEM((tok_len * group_heads, head_dim), jnp.float32),
            dma((depth, pieces)),
            dma((depth + 1, pieces)),
            dma((2, depth + 1, pieces)),
            dma((slots, pieces)),
            dma((pieces,)),
            dma((kv_heads,)),
            dma((kv_heads,)),
        ],
        compiler_params=pltpu.CompilerParams(collective_id=0, has_side_effects=True),
    )(queries, kv, doc_ids.reshape(-1, 128))
    return out.transpose(2, 0, 1, 3, 4).reshape(half, 2 * heads_here, head_dim)


def solution(mesh):
    placed = (P("ctx", "head", None), P("ctx", "head", None), P("ctx", "head", None), P())
    return jax.shard_map(
        functools.partial(body, mesh.shape["ctx"]), mesh=mesh, in_specs=placed,
        out_specs=P(("ctx", "head"), None, None), check_vma=False,
    )
```

```python
import functools
import math

import jax
import jax.numpy as jnp
from jax import lax
from jax.experimental import pallas as pl
from jax.experimental.pallas import tpu as pltpu
from jax.sharding import PartitionSpec as P

MESH = pl.DeviceIdType.MESH
MEMBERS = 4
CHUNK_BLOCKS = 4
ROWS = 512
HIDDEN = -1e30


def kernel(n, q_ref, kv_ref, docs_ref, out_ref, win, q_scr, start_tok, start_scr, done, top_scr, total_scr, sum_scr,
           ring_send, pair_send, core_send, recv, local_sem, out_send, out_recv):
    reach = n // 2 - 1
    groups = n // MEMBERS
    depth = -(-reach // MEMBERS)
    pieces = kv_ref.shape[0]
    kv_heads = pieces // 2
    tok_len = q_ref.shape[0]
    head_dim = q_ref.shape[2]
    group_heads = q_ref.shape[1] // kv_heads
    half = tok_len // 2
    scale = head_dim ** (-0.5) * math.log2(math.e)

    i = lax.axis_index("ctx")
    y = lax.axis_index("head")
    g = i // MEMBERS
    j = i % MEMBERS
    x = j // 2
    k = j % 2
    own = MEMBERS * depth + j
    first = own - reach
    after = lax.rem(i + MEMBERS, n)
    before = lax.rem(i + n - MEMBERS, n)
    pair = i + 2 - 4 * x
    sibling = i + 1 - 2 * k

    barrier = pltpu.get_barrier_semaphore()
    for target in (after, before, pair, sibling):
        pl.semaphore_signal(barrier, inc=1, device_id={"ctx": target}, device_id_type=MESH)
    pl.semaphore_signal(barrier, inc=1, device_id={"head": 1 - y}, device_id_type=MESH)
    pl.semaphore_wait(barrier, 5)

    def slot(s, m):
        return MEMBERS * (depth - s) + m

    def copy(src, lin, h, sem, target):
        return pltpu.make_async_remote_copy(
            src_ref=src, dst_ref=win.at[lin, h], send_sem=sem, recv_sem=recv.at[lin, h],
            device_id={"ctx": target}, device_id_type=MESH)

    def source(s, m, h):
        return kv_ref.at[h] if s is None else win.at[slot(s, m), h]

    base = MEMBERS * depth

    def ring_wanted(s):
        return slot(s, j) >= base - reach

    def pair_wanted(s, m, chip):
        lin = slot(s, m)
        return (lin >= base + 2 * chip - reach) & (lin < base + 2 * chip) & (g >= s)

    def core_wanted(s, m, core):
        lin = slot(s, m)
        mine = base + 2 * x + core
        return (lin >= mine - reach) & (lin < mine) & (g >= s)

    def send_ring(s, h, src, act):
        @pl.when((g + 1 < groups) & (g >= s) & ring_wanted(s + 1))
        def _():
            c = copy(src, slot(s + 1, j), h, ring_send.at[s, h], after)
            act(c)

    def send_pair(s, h, src, act):
        @pl.when(pair_wanted(s, j, 1 - x))
        def _():
            act(copy(src, slot(s, j), h, pair_send.at[s, h], pair))

    def send_core(s, m, way, h, src, act):
        @pl.when(core_wanted(s, m, 1 - k))
        def _():
            act(copy(src, slot(s, m), h, core_send.at[way, s, h], sibling))

    def start(c):
        c.start()

    def wait_sent(c):
        c.wait_send()

    def wait_slot(lin, h):
        copy(win.at[lin, h], lin, h, ring_send.at[0, h], sibling).wait_recv()

    def pump_own(h):
        send_ring(0, h, kv_ref.at[h], start)
        send_pair(0, h, kv_ref.at[h], start)
        send_core(0, j, 0, h, kv_ref.at[h], start)

    def pump_ring(s, h):
        @pl.when((g >= s) & ring_wanted(s))
        def _():
            wait_slot(slot(s, j), h)
        src = win.at[slot(s, j), h]
        if s < depth:
            send_ring(s, h, src, start)
        send_pair(s, h, src, start)
        send_core(s, j, 0, h, src, start)

    def pump_pair(s, h):
        m = j + 2 - 4 * x

        @pl.when(pair_wanted(s, m, x))
        def _():
            wait_slot(slot(s, m), h)
        send_core(s, m, 1, h, win.at[slot(s, m), h], start)

    def pump_core(s, h):
        for m in (j + 1 - 2 * k, 3 - j):
            @pl.when(core_wanted(s, m, k))
            def _():
                wait_slot(slot(s, m), h)

    def both(act, s, h):
        return [functools.partial(act, s, 2 * h), functools.partial(act, s, 2 * h + 1)]

    def stages(h):
        early = (both(pump_ring, 1, h) + both(pump_pair, 0, h) + both(pump_pair, 1, h)
                 + both(pump_core, 0, h) + both(pump_core, 1, h))
        late = []
        for s in range(2, depth + 1):
            late += [both(pump_ring, s, h), both(pump_pair, s, h)]
        late += [sum([both(pump_core, s, h) for s in range(2, depth + 1)], [])]
        return early, late

    for p in range(pieces):
        pltpu.make_async_copy(kv_ref.at[p], win.at[own, p], local_sem.at[p]).start()
    for p in range(2):
        pump_own(p)

    def clear(d, _):
        @pl.when(i < d)
        def _():
            win[own - d] = jnp.zeros(win.shape[1:], win.dtype)
        return 0
    lax.fori_loop(1, reach + 1, clear, 0)

    rows_total = tok_len * group_heads
    toks = ROWS // group_heads

    for c in range(tok_len // 128):
        ids = docs_ref[pl.ds(i * (tok_len // 128) + c, 1), :].astype(jnp.float32)
        mine = jnp.broadcast_to(ids, (128, 128)).T

        def count(r, smaller):
            other = docs_ref[pl.ds(r, 1), :].astype(jnp.float32)
            return smaller + jnp.where(other < mine, 1.0, 0.0)
        smaller = lax.fori_loop(
            0, docs_ref.shape[0], count, jnp.zeros((128, 128), jnp.float32), unroll=4)
        begin_at = jnp.sum(smaller, axis=1, keepdims=True).astype(jnp.int32)
        start_tok[pl.ds(c * 128, 128), :] = jnp.broadcast_to(begin_at, (128, 128))

    def prepare(b, _):
        t = pl.multiple_of(b * toks, toks)
        r = pl.multiple_of(b * ROWS, ROWS)
        q = q_ref[pl.ds(t, toks)].astype(jnp.float32)
        for h in range(kv_heads):
            part = q[:, h * group_heads:(h + 1) * group_heads].reshape(ROWS, head_dim)
            q_scr[h, pl.ds(r, ROWS), :] = part.astype(q_scr.dtype)
        st = start_tok[pl.ds(t, toks), :]
        start_scr[pl.ds(r, ROWS), :] = jnp.broadcast_to(
            st[:, None, :], (toks, group_heads, 128)).reshape(ROWS, 128)
        return 0
    lax.fori_loop(0, rows_total // ROWS, prepare, 0)

    chunks = (reach + 1) // CHUNK_BLOCKS
    lane = lax.broadcasted_iota(jnp.int32, (ROWS, 128), 1)
    row_tok = lax.broadcasted_iota(jnp.int32, (ROWS, 128), 0) // group_heads

    def attend(h, r, low, count, newest, state):
        q = q_scr[h, pl.ds(r, ROWS), :]
        begin = first + low
        key_base = (i - reach + low) * tok_len
        st = start_scr[pl.ds(r, ROWS), :] - key_base - lane
        tiles = []
        for b in range(count):
            keys = win[begin + b, 2 * h]
            s = lax.dot_general(q, keys, (((1,), (1,)), ((), ())),
                                preferred_element_type=jnp.float32)
            for c in range(tok_len // 128):
                off = b * tok_len + c * 128
                tile = s[:, c * 128:(c + 1) * 128]
                seen = st <= off
                if newest and b == count - 1:
                    seen = seen & (lane + c * 128 <= row_tok + r // group_heads)
                tiles.append(jnp.where(seen, tile, HIDDEN))
        top = functools.reduce(jnp.maximum, tiles)
        top = jnp.broadcast_to(jnp.max(top, axis=1, keepdims=True), (ROWS, 128))
        if state is not None:
            top = jnp.maximum(top, state[0])
        weights = [jnp.exp2((t - top) * scale) for t in tiles]
        total = functools.reduce(jnp.add, weights)
        values = win[pl.ds(begin, count), 2 * h + 1].reshape(count * tok_len, head_dim)
        packed = jnp.concatenate([w.astype(jnp.bfloat16) for w in weights], axis=1)
        product = jnp.dot(packed, values, preferred_element_type=jnp.float32)
        if state is None:
            return top, total, product
        rescale = jnp.exp2((state[0] - top) * scale)
        return top, state[1] * rescale + total, state[2] * rescale + product

    def keep(h, r, state):
        at = pl.ds(r, ROWS)
        top_scr[h, at, :] = state[0]
        total_scr[h, at, :] = state[1]
        sum_scr[h, at, :] = state[2]

    def kept(h, r):
        at = pl.ds(r, ROWS)
        return top_scr[h, at, :], total_scr[h, at, :], sum_scr[h, at, :]

    def recent(h, r):
        low = reach + 1 - CHUNK_BLOCKS
        return attend(h, r, low, CHUNK_BLOCKS - 1, False, kept(h, r))

    def own_rows(h):
        def step(b, _):
            r = pl.multiple_of(b * ROWS, ROWS)
            keep(h, r, attend(h, r, reach, 1, True, None))
            return 0
        lax.fori_loop(0, rows_total // ROWS, step, 0)

    def block(h, r):
        state = kept(h, r) if h == 0 else recent(h, r)
        if chunks == 2:
            state = attend(h, r, 0, CHUNK_BLOCKS, False, state)
        else:
            state = lax.fori_loop(
                1, chunks, lambda c, st: attend(
                    h, r, (chunks - 1 - c) * CHUNK_BLOCKS, CHUNK_BLOCKS, False, st), state)
        total = jnp.sum(state[1], axis=1, keepdims=True)
        return (state[2] / total).reshape(toks, group_heads, head_dim).astype(jnp.bfloat16)

    blocks_half = half // toks

    def rows_of(h, token0, dst, b):
        t = pl.multiple_of(token0 + b * toks, toks)
        r = pl.multiple_of(t * group_heads, ROWS)
        dst(pl.multiple_of(b * toks, toks), block(h, r))

    def store_sent(h, t, value):
        done[h, pl.ds(t, toks)] = value

    def store_own(h, t, value):
        out_ref[y, h, pl.ds(t, toks)] = value

    def out_copy(h):
        return pltpu.make_async_remote_copy(
            src_ref=done.at[h], dst_ref=out_ref.at[y, h], send_sem=out_send.at[h],
            recv_sem=out_recv.at[h], device_id={"head": 1 - y}, device_id_type=MESH)

    for p in range(pieces):
        pltpu.make_async_copy(kv_ref.at[p], win.at[own, p], local_sem.at[p]).wait()
    own_rows(0)
    early, late = stages(0)
    for number, stage in enumerate(early):
        stage()
        if number == 1:
            for p in range(2, pieces):
                pump_own(p)
            for h in range(1, kv_heads):
                own_rows(h)

    def spread(groups_of_stages, places):
        per = -(-len(groups_of_stages) // places)
        return [sum(groups_of_stages[c * per:(c + 1) * per], []) for c in range(places)]

    def whole(h):
        order = []
        for s in range(1, depth + 1):
            order += [both(pump_ring, s, h), both(pump_pair, s - 1, h)]
        order += [both(pump_pair, depth, h)]
        return order + [sum([both(pump_core, s, h) for s in range(depth + 1)], [])]

    row_blocks = rows_total // ROWS
    following = [[]] + spread(whole(1), 2 * row_blocks - 1)
    for b, now in enumerate(spread(late, row_blocks)):
        keep(0, b * ROWS, recent(0, b * ROWS))
        for stage in following[b] + now:
            stage()

    for h in range(kv_heads):
        if h == 0:
            pending = following[row_blocks:]
        elif h + 1 < kv_heads:
            pending = spread(whole(h + 1), row_blocks)
        else:
            pending = [[]] * row_blocks
        for part, (token0, store) in enumerate(
                (((1 - y) * half, store_sent), (y * half, store_own))):
            for b in range(blocks_half):
                rows_of(h, token0, functools.partial(store, h), b)
                if part == 0 and b == blocks_half - 1:
                    out_copy(h).start()
                for stage in pending[part * blocks_half + b]:
                    stage()

    for h in range(pieces):
        send_ring(0, h, kv_ref.at[h], wait_sent)
        for s in range(depth + 1):
            src = win.at[slot(s, j), h]
            if 0 < s < depth:
                send_ring(s, h, src, wait_sent)
            send_pair(s, h, src, wait_sent)
            send_core(s, j, 0, h, src, wait_sent)
            m = j + 2 - 4 * x
            send_core(s, m, 1, h, win.at[slot(s, m), h], wait_sent)
    for h in range(kv_heads):
        out_copy(h).wait()


def body(n, queries, key_rows, value_vectors, doc_ids):
    tok_len, heads_here, head_dim = queries.shape
    kv_heads = key_rows.shape[1]
    group_heads = heads_here // kv_heads
    reach = n // 2 - 1
    depth = -(-reach // MEMBERS)
    slots = MEMBERS * (depth + 1)
    kv = jnp.stack([key_rows, value_vectors]).transpose(2, 0, 1, 3)
    pieces = 2 * kv_heads
    kv = kv.reshape(pieces, tok_len, head_dim)
    half = tok_len // 2
    dma = pltpu.SemaphoreType.DMA
    out = pl.pallas_call(
        functools.partial(kernel, n),
        out_shape=jax.ShapeDtypeStruct(
            (2, kv_heads, half, group_heads, head_dim), jnp.bfloat16),
        in_specs=[pl.BlockSpec(memory_space=pltpu.VMEM)] * 3,
        out_specs=pl.BlockSpec(memory_space=pltpu.VMEM),
        scratch_shapes=[
            pltpu.VMEM((slots, pieces, tok_len, head_dim), jnp.bfloat16),
            pltpu.VMEM((kv_heads, tok_len * group_heads, head_dim), jnp.bfloat16),
            pltpu.VMEM((tok_len, 128), jnp.int32),
            pltpu.VMEM((tok_len * group_heads, 128), jnp.int32),
            pltpu.VMEM((kv_heads, half, group_heads, head_dim), jnp.bfloat16),
            pltpu.VMEM((kv_heads, tok_len * group_heads, 128), jnp.float32),
            pltpu.VMEM((kv_heads, tok_len * group_heads, 128), jnp.float32),
            pltpu.VMEM((kv_heads, tok_len * group_heads, head_dim), jnp.float32),
            dma((depth, pieces)),
            dma((depth + 1, pieces)),
            dma((2, depth + 1, pieces)),
            dma((slots, pieces)),
            dma((pieces,)),
            dma((kv_heads,)),
            dma((kv_heads,)),
        ],
        compiler_params=pltpu.CompilerParams(collective_id=0, has_side_effects=True),
    )(queries, kv, doc_ids.reshape(-1, 128))
    return out.transpose(2, 0, 1, 3, 4).reshape(half, 2 * heads_here, head_dim)


def solution(mesh):
    placed = (P("ctx", "head", None), P("ctx", "head", None), P("ctx", "head", None), P())
    return jax.shard_map(
        functools.partial(body, mesh.shape["ctx"]), mesh=mesh, in_specs=placed,
        out_specs=P(("ctx", "head"), None, None), check_vma=False,
    )
```

```python
import functools
import math

import jax
import jax.numpy as jnp
from jax import lax
from jax.experimental import pallas as pl
from jax.experimental.pallas import tpu as pltpu
from jax.sharding import PartitionSpec as P

MESH = pl.DeviceIdType.MESH
MEMBERS = 4
CHUNK_BLOCKS = 4
ROWS = 512
HIDDEN = -1e30


def kernel(n, q_ref, kv_ref, docs_ref, out_ref, win, q_scr, start_tok, start_scr, done, top_scr, total_scr, sum_scr,
           ring_send, pair_send, core_send, recv, local_sem, out_send, out_recv):
    reach = n // 2 - 1
    groups = n // MEMBERS
    depth = -(-reach // MEMBERS)
    pieces = kv_ref.shape[0]
    kv_heads = pieces // 2
    tok_len = q_ref.shape[0]
    head_dim = q_ref.shape[2]
    group_heads = q_ref.shape[1] // kv_heads
    half = tok_len // 2
    scale = head_dim ** (-0.5) * math.log2(math.e)

    i = lax.axis_index("ctx")
    y = lax.axis_index("head")
    g = i // MEMBERS
    j = i % MEMBERS
    x = j // 2
    k = j % 2
    own = MEMBERS * depth + j
    first = own - reach
    after = lax.rem(i + MEMBERS, n)
    before = lax.rem(i + n - MEMBERS, n)
    pair = i + 2 - 4 * x
    sibling = i + 1 - 2 * k

    barrier = pltpu.get_barrier_semaphore()
    for target in (after, before, pair, sibling):
        pl.semaphore_signal(barrier, inc=1, device_id={"ctx": target}, device_id_type=MESH)
    pl.semaphore_signal(barrier, inc=1, device_id={"head": 1 - y}, device_id_type=MESH)
    pl.semaphore_wait(barrier, 5)

    def slot(s, m):
        return MEMBERS * (depth - s) + m

    def copy(src, lin, h, sem, target):
        return pltpu.make_async_remote_copy(
            src_ref=src, dst_ref=win.at[lin, h], send_sem=sem, recv_sem=recv.at[lin, h],
            device_id={"ctx": target}, device_id_type=MESH)

    def source(s, m, h):
        return kv_ref.at[h] if s is None else win.at[slot(s, m), h]

    base = MEMBERS * depth

    def ring_wanted(s):
        return slot(s, j) >= base - reach

    def pair_wanted(s, m, chip):
        lin = slot(s, m)
        return (lin >= base + 2 * chip - reach) & (lin < base + 2 * chip) & (g >= s)

    def core_wanted(s, m, core):
        lin = slot(s, m)
        mine = base + 2 * x + core
        return (lin >= mine - reach) & (lin < mine) & (g >= s)

    def send_ring(s, h, src, act):
        @pl.when((g + 1 < groups) & (g >= s) & ring_wanted(s + 1))
        def _():
            c = copy(src, slot(s + 1, j), h, ring_send.at[s, h], after)
            act(c)

    def send_pair(s, h, src, act):
        @pl.when(pair_wanted(s, j, 1 - x))
        def _():
            act(copy(src, slot(s, j), h, pair_send.at[s, h], pair))

    def send_core(s, m, way, h, src, act):
        @pl.when(core_wanted(s, m, 1 - k))
        def _():
            act(copy(src, slot(s, m), h, core_send.at[way, s, h], sibling))

    def start(c):
        c.start()

    def wait_sent(c):
        c.wait_send()

    def wait_slot(lin, h):
        copy(win.at[lin, h], lin, h, ring_send.at[0, h], sibling).wait_recv()

    def pump_own(h):
        send_ring(0, h, kv_ref.at[h], start)
        send_pair(0, h, kv_ref.at[h], start)
        send_core(0, j, 0, h, kv_ref.at[h], start)

    def pump_ring(s, h):
        @pl.when((g >= s) & ring_wanted(s))
        def _():
            wait_slot(slot(s, j), h)
        src = win.at[slot(s, j), h]
        if s < depth:
            send_ring(s, h, src, start)
        send_pair(s, h, src, start)
        send_core(s, j, 0, h, src, start)

    def pump_pair(s, h):
        m = j + 2 - 4 * x

        @pl.when(pair_wanted(s, m, x))
        def _():
            wait_slot(slot(s, m), h)
        send_core(s, m, 1, h, win.at[slot(s, m), h], start)

    def pump_core(s, h):
        for m in (j + 1 - 2 * k, 3 - j):
            @pl.when(core_wanted(s, m, k))
            def _():
                wait_slot(slot(s, m), h)

    def both(act, s, h):
        return [functools.partial(act, s, 2 * h), functools.partial(act, s, 2 * h + 1)]

    def stages(h):
        early = (both(pump_ring, 1, h) + both(pump_pair, 0, h) + both(pump_pair, 1, h)
                 + both(pump_core, 0, h) + both(pump_core, 1, h))
        late = []
        for s in range(2, depth + 1):
            late += [both(pump_ring, s, h), both(pump_pair, s, h)]
        late += [sum([both(pump_core, s, h) for s in range(2, depth + 1)], [])]
        return early, late

    for p in range(pieces):
        pltpu.make_async_copy(kv_ref.at[p], win.at[own, p], local_sem.at[p]).start()
    for p in range(2):
        pump_own(p)

    def clear(d, _):
        @pl.when(i < d)
        def _():
            win[own - d] = jnp.zeros(win.shape[1:], win.dtype)
        return 0
    lax.fori_loop(1, reach + 1, clear, 0)

    rows_total = tok_len * group_heads
    toks = ROWS // group_heads

    for c in range(tok_len // 128):
        ids = docs_ref[pl.ds(i * (tok_len // 128) + c, 1), :].astype(jnp.float32)
        mine = jnp.broadcast_to(ids, (128, 128)).T

        def count(r, smaller):
            other = docs_ref[pl.ds(r, 1), :].astype(jnp.float32)
            return smaller + jnp.where(other < mine, 1.0, 0.0)
        smaller = lax.fori_loop(
            0, docs_ref.shape[0], count, jnp.zeros((128, 128), jnp.float32), unroll=4)
        begin_at = jnp.sum(smaller, axis=1, keepdims=True).astype(jnp.int32)
        start_tok[pl.ds(c * 128, 128), :] = jnp.broadcast_to(begin_at, (128, 128))

    def prepare(b, _):
        t = pl.multiple_of(b * toks, toks)
        r = pl.multiple_of(b * ROWS, ROWS)
        q = q_ref[pl.ds(t, toks)].astype(jnp.float32)
        for h in range(kv_heads):
            part = q[:, h * group_heads:(h + 1) * group_heads].reshape(ROWS, head_dim)
            q_scr[h, pl.ds(r, ROWS), :] = part.astype(q_scr.dtype)
        st = start_tok[pl.ds(t, toks), :]
        start_scr[pl.ds(r, ROWS), :] = jnp.broadcast_to(
            st[:, None, :], (toks, group_heads, 128)).reshape(ROWS, 128)
        return 0
    lax.fori_loop(0, rows_total // ROWS, prepare, 0)

    chunks = (reach + 1) // CHUNK_BLOCKS
    lane = lax.broadcasted_iota(jnp.int32, (ROWS, 128), 1)
    row_tok = lax.broadcasted_iota(jnp.int32, (ROWS, 128), 0) // group_heads

    def attend(h, r, low, count, newest, state):
        q = q_scr[h, pl.ds(r, ROWS), :]
        begin = first + low
        key_base = (i - reach + low) * tok_len
        st = start_scr[pl.ds(r, ROWS), :] - key_base - lane
        tiles = []
        for b in range(count):
            keys = win[begin + b, 2 * h]
            s = lax.dot_general(q, keys, (((1,), (1,)), ((), ())),
                                preferred_element_type=jnp.float32)
            for c in range(tok_len // 128):
                off = b * tok_len + c * 128
                tile = s[:, c * 128:(c + 1) * 128]
                seen = st <= off
                if newest and b == count - 1:
                    seen = seen & (lane + c * 128 <= row_tok + r // group_heads)
                tiles.append(jnp.where(seen, tile, HIDDEN))
        top = functools.reduce(jnp.maximum, tiles)
        top = jnp.broadcast_to(jnp.max(top, axis=1, keepdims=True), (ROWS, 128))
        if state is not None:
            top = jnp.maximum(top, state[0])
        weights = [jnp.exp2((t - top) * scale) for t in tiles]
        total = functools.reduce(jnp.add, weights)
        values = win[pl.ds(begin, count), 2 * h + 1].reshape(count * tok_len, head_dim)
        packed = jnp.concatenate([w.astype(jnp.bfloat16) for w in weights], axis=1)
        product = jnp.dot(packed, values, preferred_element_type=jnp.float32)
        if state is None:
            return top, total, product
        rescale = jnp.exp2((state[0] - top) * scale)
        return top, state[1] * rescale + total, state[2] * rescale + product

    def keep(h, r, state):
        at = pl.ds(r, ROWS)
        top_scr[h, at, :] = state[0]
        total_scr[h, at, :] = state[1]
        sum_scr[h, at, :] = state[2]

    def kept(h, r):
        at = pl.ds(r, ROWS)
        return top_scr[h, at, :], total_scr[h, at, :], sum_scr[h, at, :]

    def recent(h, r):
        low = reach + 1 - CHUNK_BLOCKS
        return attend(h, r, low, CHUNK_BLOCKS - 1, False, kept(h, r))

    def own_rows(h):
        def step(b, _):
            r = pl.multiple_of(b * ROWS, ROWS)
            keep(h, r, attend(h, r, reach, 1, True, None))
            return 0
        lax.fori_loop(0, rows_total // ROWS, step, 0)

    def block(h, r):
        state = kept(h, r) if h == 0 else recent(h, r)
        if chunks == 2:
            state = attend(h, r, 0, CHUNK_BLOCKS, False, state)
        else:
            state = lax.fori_loop(
                1, chunks, lambda c, st: attend(
                    h, r, (chunks - 1 - c) * CHUNK_BLOCKS, CHUNK_BLOCKS, False, st), state)
        total = jnp.sum(state[1], axis=1, keepdims=True)
        return (state[2] / total).reshape(toks, group_heads, head_dim).astype(jnp.bfloat16)

    blocks_half = half // toks

    def rows_of(h, token0, dst, b):
        t = pl.multiple_of(token0 + b * toks, toks)
        r = pl.multiple_of(t * group_heads, ROWS)
        dst(pl.multiple_of(b * toks, toks), block(h, r))

    def store_sent(h, t, value):
        done[h, pl.ds(t, toks)] = value

    def store_own(h, t, value):
        out_ref[y, h, pl.ds(t, toks)] = value

    def out_copy(h):
        return pltpu.make_async_remote_copy(
            src_ref=done.at[h], dst_ref=out_ref.at[y, h], send_sem=out_send.at[h],
            recv_sem=out_recv.at[h], device_id={"head": 1 - y}, device_id_type=MESH)

    for p in range(pieces):
        pltpu.make_async_copy(kv_ref.at[p], win.at[own, p], local_sem.at[p]).wait()
    own_rows(0)
    early, late = stages(0)
    for number, stage in enumerate(early):
        stage()
        if number == 1:
            for p in range(2, pieces):
                pump_own(p)
        if number == 3:
            for h in range(1, kv_heads):
                own_rows(h)

    def spread(groups_of_stages, places):
        per = -(-len(groups_of_stages) // places)
        return [sum(groups_of_stages[c * per:(c + 1) * per], []) for c in range(places)]

    def whole(h):
        order = []
        for s in range(1, depth + 1):
            order += [both(pump_ring, s, h), both(pump_pair, s - 1, h)]
        order += [both(pump_pair, depth, h)]
        return order + [sum([both(pump_core, s, h) for s in range(depth + 1)], [])]

    row_blocks = rows_total // ROWS
    following = [[]] + spread(whole(1), 2 * row_blocks - 1)
    for b, now in enumerate(spread(late, row_blocks)):
        keep(0, b * ROWS, recent(0, b * ROWS))
        for stage in following[b] + now:
            stage()

    for h in range(kv_heads):
        if h == 0:
            pending = following[row_blocks:]
        elif h + 1 < kv_heads:
            pending = spread(whole(h + 1), row_blocks)
        else:
            pending = [[]] * row_blocks
        for part, (token0, store) in enumerate(
                (((1 - y) * half, store_sent), (y * half, store_own))):
            for b in range(blocks_half):
                rows_of(h, token0, functools.partial(store, h), b)
                if part == 0 and b == blocks_half - 1:
                    out_copy(h).start()
                for stage in pending[part * blocks_half + b]:
                    stage()

    for h in range(pieces):
        send_ring(0, h, kv_ref.at[h], wait_sent)
        for s in range(depth + 1):
            src = win.at[slot(s, j), h]
            if 0 < s < depth:
                send_ring(s, h, src, wait_sent)
            send_pair(s, h, src, wait_sent)
            send_core(s, j, 0, h, src, wait_sent)
            m = j + 2 - 4 * x
            send_core(s, m, 1, h, win.at[slot(s, m), h], wait_sent)
    for h in range(kv_heads):
        out_copy(h).wait()


def body(n, queries, key_rows, value_vectors, doc_ids):
    tok_len, heads_here, head_dim = queries.shape
    kv_heads = key_rows.shape[1]
    group_heads = heads_here // kv_heads
    reach = n // 2 - 1
    depth = -(-reach // MEMBERS)
    slots = MEMBERS * (depth + 1)
    kv = jnp.stack([key_rows, value_vectors]).transpose(2, 0, 1, 3)
    pieces = 2 * kv_heads
    kv = kv.reshape(pieces, tok_len, head_dim)
    half = tok_len // 2
    dma = pltpu.SemaphoreType.DMA
    out = pl.pallas_call(
        functools.partial(kernel, n),
        out_shape=jax.ShapeDtypeStruct(
            (2, kv_heads, half, group_heads, head_dim), jnp.bfloat16),
        in_specs=[pl.BlockSpec(memory_space=pltpu.VMEM)] * 3,
        out_specs=pl.BlockSpec(memory_space=pltpu.VMEM),
        scratch_shapes=[
            pltpu.VMEM((slots, pieces, tok_len, head_dim), jnp.bfloat16),
            pltpu.VMEM((kv_heads, tok_len * group_heads, head_dim), jnp.bfloat16),
            pltpu.VMEM((tok_len, 128), jnp.int32),
            pltpu.VMEM((tok_len * group_heads, 128), jnp.int32),
            pltpu.VMEM((kv_heads, half, group_heads, head_dim), jnp.bfloat16),
            pltpu.VMEM((kv_heads, tok_len * group_heads, 128), jnp.float32),
            pltpu.VMEM((kv_heads, tok_len * group_heads, 128), jnp.float32),
            pltpu.VMEM((kv_heads, tok_len * group_heads, head_dim), jnp.float32),
            dma((depth, pieces)),
            dma((depth + 1, pieces)),
            dma((2, depth + 1, pieces)),
            dma((slots, pieces)),
            dma((pieces,)),
            dma((kv_heads,)),
            dma((kv_heads,)),
        ],
        compiler_params=pltpu.CompilerParams(collective_id=0, has_side_effects=True),
    )(queries, kv, doc_ids.reshape(-1, 128))
    return out.transpose(2, 0, 1, 3, 4).reshape(half, 2 * heads_here, head_dim)


def solution(mesh):
    placed = (P("ctx", "head", None), P("ctx", "head", None), P("ctx", "head", None), P())
    return jax.shard_map(
        functools.partial(body, mesh.shape["ctx"]), mesh=mesh, in_specs=placed,
        out_specs=P(("ctx", "head"), None, None), check_vma=False,
    )
```
